32 devices in a mesh: gx: 4 (over y, x), gy: 8 (over z, core).
Axes of the slice: x: 2, y: 2, z: 4, core: 2. Of those that a mesh axis runs over, the one named last changes fastest.
Arguments:
- density_one: float32 [512, 512, 512], P('gx', 'gy'), may hold values from -6 to 6
- density_two: float32 [512, 512, 512], P('gx', 'gy'), may hold values from -6 to 6
Outputs:
- correlation: float32 [512, 512, 512], P('gx', 'gy')
The draws below stay inside these ranges and needn't reach their ends.
All inputs are finite; a program needn't handle non-finite values.
Results may differ from the reference program's by a relative error of at most 0.00013.
Values sent between devices are 32-bit elements; how exact they have to be, the bound alone decides.
A program may use at most 256 MiB of HBM per device.

```python
import math
import jax
import jax.numpy as jnp

NX = 512
NY = 512
NZ = 512


def levels(stream_key, extent, pieces, low, largest):
    def one(position, parts):
        steps = jax.random.uniform(jax.random.fold_in(jax.random.fold_in(stream_key, 6), position), (parts,), jnp.float32, low / len(pieces), largest / len(pieces))
        return jnp.repeat(jnp.exp(steps), extent[position] // parts).reshape((-1,) + (1,) * (len(extent) - position - 1))

    level = one(*pieces[0])
    for cut in pieces[1:]:
        level = level * one(*cut)
    return level


def normal_values(own_key, extent, scale, reach, cuts=(), kind=jnp.bfloat16):
    result = scale * jax.random.normal(own_key, extent, jnp.float32)
    if cuts:
        result = result * levels(own_key, extent, cuts, -0.22, 0.18)
    return jnp.clip(result, -reach, reach).astype(kind)


def setup_inputs(seed: int = 0) -> dict:
    arg_keys = jax.random.split(jax.random.key(seed), 3)
    return {
        "density_one": normal_values(arg_keys[0], (NX, NY, NZ), 1.0, 6.0, ((0, 4), (1, 8)), jnp.float32),
        "density_two": normal_values(arg_keys[1], (NX, NY, NZ), 1.0, 6.0, ((0, 4), (1, 8)), jnp.float32),
    }


def reference(density_one, density_two):
    cell_total = NX * NY * NZ
    spectrum_one = jnp.fft.rfftn(density_one)
    spectrum_two = jnp.fft.rfftn(density_two)
    power = (spectrum_one.real * spectrum_two.real + spectrum_one.imag * spectrum_two.imag) / cell_total
    wave_x = jnp.arange(NX)[:, None, None]
    wave_y = jnp.arange(NY)[None, :, None]
    wave_z = jnp.arange(NZ // 2 + 1)[None, None, :]
    kept_modes = (wave_x != NX // 2) & (wave_y != NY // 2) & (wave_z != NZ // 2)
    power = jnp.where(kept_modes, power, jnp.zeros_like(power))
    correlation = jnp.fft.irfftn(power * (1.0 + 0j), s=(NX, NY, NZ)) * math.sqrt(cell_total)
    return correlation.astype(jnp.float32)
```

```python
import functools
import math

import jax
import jax.numpy as jnp
import numpy as np
from jax import lax
from jax.experimental import pallas as pl
from jax.experimental.pallas import tpu as pltpu
from jax.sharding import PartitionSpec as P

MESH = pl.DeviceIdType.MESH
GROUP = 8
LANES = 128
f32 = jnp.float32
bf16 = jnp.bfloat16


def trig(length):
    positions = np.arange(length)
    radians = (positions[:, None] * positions[None, :] % length) * (2.0 * math.pi / length)
    return np.concatenate([np.cos(radians), np.sin(radians)]).astype(np.float32)


def halves(table):
    table = jnp.asarray(table)
    high = table.astype(bf16)
    low = (table - high.astype(f32)).astype(bf16)
    return high, low


def split(values):
    high = values.astype(bf16)
    return high, (values - high.astype(f32)).astype(bf16)


def dot3(left, right, contract):
    def one(a, b):
        return lax.dot_general(a, b, (contract, ((), ())), preferred_element_type=f32)

    (lh, ll), (rh, rl) = left, right
    return one(lh, rh) + one(lh, rl) + one(ll, rh)


def build_rotation(table, out, size, right):
    for part in range(2):
        cos = table[part][0:size, :]
        sin = table[part][size : 2 * size, :]
        out[part][0:size, 0:size] = cos
        out[part][size : 2 * size, size : 2 * size] = cos
        out[part][0:size, size : 2 * size] = -sin if right else sin
        out[part][size : 2 * size, 0:size] = sin if right else -sin


def exchange_kernel(sizes, *refs):
    (count_x, count_y, x_local, y_local, depth, compute) = sizes
    devices = count_x * count_y
    grid_x, grid_y = count_x * x_local, count_y * y_local
    half = depth // 2
    slices = half // devices
    pack = LANES // x_local
    span = GROUP * pack
    groups = y_local // span
    cell_total = float(grid_x * grid_y * depth)
    (d1, d2, xc, xcl, yc_, ycl, zc, zcl,
     back, z1, z2, r1, r2, bs,
     dt, zt, rxh, rxl, ryh, ryl, xh, xl, lh, ll, spec, ph, plo, gh, gl, bt, pf,
     local, sent, got) = refs
    gx, gy = lax.axis_index("gx"), lax.axis_index("gy")
    me = gx * count_y + gy

    def peer(offset):
        dest = lax.rem(me + offset, devices)
        return dest, (dest // count_y, lax.rem(dest, count_y))

    barrier = pltpu.get_barrier_semaphore()

    def greet(offset, _):
        pl.semaphore_signal(barrier, inc=1, device_id=peer(offset)[1], device_id_type=MESH)
        return 0

    lax.fori_loop(1, devices, greet, 0)

    def local_copy(src, dst):
        copy = pltpu.make_async_copy(src, dst, local)
        copy.start()
        copy.wait()

    def send_all(source, target, sem):
        own = pltpu.make_async_copy(source(me), target, got.at[sem])
        own.start()

        def one(offset, _):
            dest, where = peer(offset)
            pltpu.make_async_remote_copy(
                source(dest), target, sent.at[sem], got.at[sem],
                device_id=where, device_id_type=MESH,
            ).start()
            return 0

        lax.fori_loop(1, devices, one, 0)

    def wait_bytes(ref, sem):
        pltpu.make_async_copy(ref, ref, sem).wait()

    rows_all = slices * devices * 2 * GROUP
    depth_tiles = depth // LANES

    def depth_forward(density, z, group):
        for tile in range(depth_tiles):
            pltpu.make_async_copy(
                density.at[:, pl.ds(group * span, span), pl.ds(tile * LANES, LANES)], dt.at[tile], local
            ).start()
        pltpu.make_async_copy(dt, dt, local).wait()
        if compute:
            lines = dt.reshape(depth_tiles * x_local * span, LANES)
            out = zt.reshape(rows_all, LANES)
            for first in range(0, GROUP, 2):
                cells = jnp.concatenate(
                    [
                        jnp.concatenate(
                            [
                                lines[pl.ds(tile * x_local * span + h * GROUP + row, x_local, stride=span), :]
                                for tile in range(depth_tiles)
                            ],
                            axis=1,
                        )
                        for row in (first, first + 1)
                        for h in range(pack)
                    ],
                    axis=0,
                )
                cells = split(cells)
                for c in range(2):
                    table = (zc[c * depth : c * depth + half, :], zcl[c * depth : c * depth + half, :])
                    rows = dot3(table, cells, ((1,), (1,)))
                    if c:
                        rows = -rows
                    for n in range(2):
                        out[pl.ds(c * GROUP + first + n, half, stride=2 * GROUP), :] = rows[
                            :, n * LANES : (n + 1) * LANES
                        ]
        local_copy(zt, z.at[:, :, group])

    def first_field(group, _):
        depth_forward(d1, z1, group)

        @pl.when(group == 0)
        def _():
            pl.semaphore_wait(barrier, devices - 1)

        send_all(lambda dest: z1.at[:, dest, group], r1.at[:, me, group], group)
        return 0

    lax.fori_loop(0, groups, first_field, 0)

    def second_field(group, _):
        depth_forward(d2, z2, group)
        return 0

    lax.fori_loop(0, groups, second_field, 0)
    if compute:
        build_rotation((xc, xcl), (rxh, rxl), grid_x, True)
        build_rotation((yc_, ycl), (ryh, ryl), grid_y, False)

    def unpack_rows(block):
        if pack > 1:
            block = jnp.concatenate(
                [
                    block[..., h * x_local : (h + 1) * x_local].reshape(count_y, groups, 1, GROUP, x_local)
                    for h in range(pack)
                ],
                axis=2,
            )
        return block.reshape(grid_y, x_local)

    def pack_rows(block):
        if pack == 1:
            return block.reshape(count_y, groups, GROUP, x_local)
        block = block.reshape(count_y, groups, pack, GROUP, x_local)
        return jnp.concatenate([block[:, :, h] for h in range(pack)], axis=-1)

    waited = 0
    for k in range(slices):
        upto = (k + 1) * groups // slices
        for group in range(waited, upto):
            wait_bytes(r1.at[:, :, group], got.at[group])
        waited = upto
        send_all(lambda dest: z2.at[k, dest], r2.at[k, me], groups + k)

    tile_x = min(256, grid_x)
    tile_y = min(256, grid_y)
    ky = lax.broadcasted_iota(jnp.int32, (grid_y, grid_x), 0)
    kx = lax.broadcasted_iota(jnp.int32, (grid_y, grid_x), 1)
    keep = (ky != grid_y // 2) & (kx != grid_x // 2)

    def plane(k, _):
        wait_bytes(r2.at[k], got.at[groups + k])
        local_copy(r1.at[k], pf.at[0])
        local_copy(r2.at[k], pf.at[1])
        if compute:
            def forward(field, _):
                cells = pf.at[field].reshape(count_x, count_y, groups, 2, GROUP, LANES)
                for c in range(2):
                    for i in range(count_x):
                        high, low = split(unpack_rows(cells[i, :, :, c]))
                        at = c * grid_x + i * x_local
                        xh[:, at : at + x_local] = high
                        xl[:, at : at + x_local] = low
                for n in range(2 * grid_x // tile_x):
                    cols = slice(n * tile_x, (n + 1) * tile_x)
                    part = dot3((xh[...], xl[...]), (rxh[:, cols], rxl[:, cols]), ((1,), (0,)))
                    c, at = divmod(n * tile_x, grid_x)
                    high, low = split(part)
                    lh[c * grid_y : (c + 1) * grid_y, at : at + tile_x] = high
                    ll[c * grid_y : (c + 1) * grid_y, at : at + tile_x] = low
                for m in range(2 * grid_y // tile_y):
                    rows = slice(m * tile_y, (m + 1) * tile_y)
                    spec[field, rows, :] = dot3((ryh[rows, :], ryl[rows, :]), (lh[...], ll[...]), ((1,), (0,)))
                return 0

            lax.fori_loop(0, 2, forward, 0)
            power = spec[0, 0:grid_y] * spec[1, 0:grid_y] + spec[0, grid_y:] * spec[1, grid_y:]
            weight = jnp.where((k == 0) & (me == 0), 1.0, 2.0).astype(f32) * (1.0 / math.sqrt(cell_total))
            power = jnp.where(keep, power / cell_total, 0.0) * weight
            ph[...], plo[...] = split(power)
            for m in range(2 * grid_y // tile_y):
                rows = slice(m * tile_y, (m + 1) * tile_y)
                part = dot3((yc_[rows, :], ycl[rows, :]), (ph[...], plo[...]), ((1,), (0,)))
                c, at = divmod(m * tile_y, grid_y)
                high, low = split(part)
                gh[at : at + tile_y, c * grid_x : (c + 1) * grid_x] = high
                gl[at : at + tile_y, c * grid_x : (c + 1) * grid_x] = low
            cells = bt.reshape(count_x, count_y, groups, 2, GROUP, LANES)
            for n in range(2 * grid_x // tile_x):
                rows = slice(n * tile_x, (n + 1) * tile_x)
                part = dot3((gh[...], gl[...]), (rxh[rows, :], rxl[rows, :]), ((1,), (1,)))
                c, at = divmod(n * tile_x, grid_x)
                for m in range(tile_x // x_local):
                    i = at // x_local + m
                    cells[i, :, :, c] = pack_rows(part[:, m * x_local : (m + 1) * x_local])
        local_copy(bt, bs.at[k])
        send_all(lambda dest: bs.at[k, dest], back.at[k, me], groups + slices + k)
        return 0

    lax.fori_loop(0, slices, plane, 0)
    for k in range(slices):
        wait_bytes(back.at[k], got.at[groups + slices + k])
    for group in range(groups):
        wait_bytes(z1.at[:, pl.ds(0, devices - 1), group], sent.at[group])
    for k in range(slices):
        wait_bytes(z2.at[k, pl.ds(0, devices - 1)], sent.at[groups + k])
        wait_bytes(bs.at[k, pl.ds(0, devices - 1)], sent.at[groups + slices + k])


def depth_inverse_kernel(x_local, depth, groups, rows_ref, high_ref, low_ref, out_ref, block, done):
    half = depth // 2
    pack = LANES // x_local
    span = GROUP * pack
    depth_tiles = depth // LANES
    rows = rows_ref.reshape(half * 2 * GROUP, LANES)
    group = pl.program_id(0)
    slot = lax.rem(group, 2)

    def finish(slot):
        pltpu.make_async_copy(block.at[slot], block.at[slot], done.at[slot]).wait()

    @pl.when(group >= 2)
    def _():
        finish(slot)

    out = block.at[slot].reshape(depth_tiles * x_local * span, LANES)
    for first in range(0, GROUP, 2):
        total = None
        for c in range(2):
            lines = jnp.concatenate(
                [rows[pl.ds(c * GROUP + first + n, half, stride=2 * GROUP), :] for n in range(2)], axis=1
            )
            table = (
                high_ref[c * depth : c * depth + half, :],
                low_ref[c * depth : c * depth + half, :],
            )
            part = dot3(split(lines), table, ((0,), (0,)))
            total = part if c == 0 else total - part
        for n in range(2):
            for h in range(pack):
                at = n * LANES + h * x_local
                for tile in range(depth_tiles):
                    out[pl.ds(tile * x_local * span + h * GROUP + first + n, x_local, stride=span), :] = total[
                        at : at + x_local, tile * LANES : (tile + 1) * LANES
                    ]
    for tile in range(depth_tiles):
        pltpu.make_async_copy(
            block.at[slot, tile],
            out_ref.at[:, pl.ds(group * span, span), pl.ds(tile * LANES, LANES)],
            done.at[slot],
        ).start()

    @pl.when(group == groups - 1)
    def _():
        for other in range(min(2, groups)):
            finish(other)


def on_device(compute, density_one, density_two):
    count_x = lax.axis_size("gx")
    count_y = lax.axis_size("gy")
    devices = count_x * count_y
    x_local, y_local, depth = density_one.shape
    grid_x, grid_y = x_local * count_x, y_local * count_y
    slices = depth // 2 // devices
    span = GROUP * (LANES // x_local)
    groups = y_local // span
    tables = {length: halves(trig(length)) for length in {grid_x, grid_y, depth}}
    packed = jax.ShapeDtypeStruct((slices, devices, groups, 2 * GROUP, LANES), f32)
    vmem = pl.BlockSpec(memory_space=pltpu.VMEM)
    hbm = pl.BlockSpec(memory_space=pl.ANY)
    scratch = [
        pltpu.VMEM((depth // LANES, x_local, span, LANES), f32),
        pltpu.VMEM((slices, devices, 2 * GROUP, LANES), f32),
        pltpu.VMEM((2 * grid_x, 2 * grid_x), bf16),
        pltpu.VMEM((2 * grid_x, 2 * grid_x), bf16),
        pltpu.VMEM((2 * grid_y, 2 * grid_y), bf16),
        pltpu.VMEM((2 * grid_y, 2 * grid_y), bf16),
        pltpu.VMEM((grid_y, 2 * grid_x), bf16),
        pltpu.VMEM((grid_y, 2 * grid_x), bf16),
        pltpu.VMEM((2 * grid_y, grid_x), bf16),
        pltpu.VMEM((2 * grid_y, grid_x), bf16),
        pltpu.VMEM((2, 2 * grid_y, grid_x), f32),
        pltpu.VMEM((grid_y, grid_x), bf16),
        pltpu.VMEM((grid_y, grid_x), bf16),
        pltpu.VMEM((grid_y, 2 * grid_x), bf16),
        pltpu.VMEM((grid_y, 2 * grid_x), bf16),
        pltpu.VMEM((devices, groups, 2 * GROUP, LANES), f32),
        pltpu.VMEM((2, devices, groups, 2 * GROUP, LANES), f32),
        pltpu.SemaphoreType.DMA,
        pltpu.SemaphoreType.DMA((groups + 2 * slices,)),
        pltpu.SemaphoreType.DMA((groups + 2 * slices,)),
    ]
    sizes = (count_x, count_y, x_local, y_local, depth, compute)
    back = pl.pallas_call(
        functools.partial(exchange_kernel, sizes),
        out_shape=[packed] * 6,
        in_specs=[hbm] * 2 + [vmem] * 6,
        out_specs=[hbm] * 6,
        scratch_shapes=scratch,
        compiler_params=pltpu.CompilerParams(
            collective_id=0, has_side_effects=True, vmem_limit_bytes=60 * 2**20
        ),
    )(density_one, density_two, *tables[grid_x], *tables[grid_y], *tables[depth])[0]
    return pl.pallas_call(
        functools.partial(depth_inverse_kernel, x_local, depth, groups),
        grid=(groups,),
        out_shape=jax.ShapeDtypeStruct(density_one.shape, f32),
        in_specs=[
            pl.BlockSpec((slices, devices, 1, 2 * GROUP, LANES), lambda g: (0, 0, g, 0, 0)),
            pl.BlockSpec((2 * depth, depth), lambda g: (0, 0)),
            pl.BlockSpec((2 * depth, depth), lambda g: (0, 0)),
        ],
        out_specs=hbm,
        scratch_shapes=[
            pltpu.VMEM((2, depth // LANES, x_local, span, LANES), f32),
            pltpu.SemaphoreType.DMA((2,)),
        ],
        compiler_params=pltpu.CompilerParams(vmem_limit_bytes=48 * 2**20),
    )(back, *tables[depth])


def solution(mesh, compute=True):
    return jax.shard_map(
        functools.partial(on_device, compute),
        mesh=mesh,
        in_specs=(P("gx", "gy", None), P("gx", "gy", None)),
        out_specs=P("gx", "gy", None),
        check_vma=False,
    )
```

```python
import functools
import math

import jax
import jax.numpy as jnp
import numpy as np
from jax import lax
from jax.experimental import pallas as pl
from jax.experimental.pallas import tpu as pltpu
from jax.sharding import PartitionSpec as P

MESH = pl.DeviceIdType.MESH
GROUP = 8
LANES = 128
f32 = jnp.float32
bf16 = jnp.bfloat16


def trig(length):
    positions = np.arange(length)
    radians = (positions[:, None] * positions[None, :] % length) * (2.0 * math.pi / length)
    return np.concatenate([np.cos(radians), np.sin(radians)]).astype(np.float32)


def halves(table):
    table = jnp.asarray(table)
    high = table.astype(bf16)
    low = (table - high.astype(f32)).astype(bf16)
    return high, low


def split(values):
    high = values.astype(bf16)
    return high, (values - high.astype(f32)).astype(bf16)


def dot3(left, right, contract):
    def one(a, b):
        return lax.dot_general(a, b, (contract, ((), ())), preferred_element_type=f32)

    (lh, ll), (rh, rl) = left, right
    return one(lh, rh) + one(lh, rl) + one(ll, rh)


def build_rotation(table, out, size, right):
    for part in range(2):
        cos = table[part][0:size, :]
        sin = table[part][size : 2 * size, :]
        out[part][0:size, 0:size] = cos
        out[part][size : 2 * size, size : 2 * size] = cos
        out[part][0:size, size : 2 * size] = -sin if right else sin
        out[part][size : 2 * size, 0:size] = sin if right else -sin


def interleave(lines, count, x_local, span, out):
    for row in range(GROUP):
        cells = jnp.concatenate(
            [lines[pl.ds(c * GROUP + row, count, stride=2 * GROUP), :] for c in range(2)], axis=0
        ).T
        for h in range(span // GROUP):
            for tile in range(2 * count // LANES):
                out[pl.ds(tile * x_local * span + h * GROUP + row, x_local, stride=span), :] = cells[
                    h * x_local : (h + 1) * x_local, tile * LANES : (tile + 1) * LANES
                ]


def interleaved_rows(lines, rows):
    return split(jnp.concatenate([lines[tile, rows, :] for tile in range(lines.shape[0])], axis=1))


def tail_slices(slices):
    return max(1, slices // 4)


def exchange_kernel(sizes, *refs):
    count_x, count_y, x_local, y_local, depth = sizes
    devices = count_x * count_y
    grid_x, grid_y = count_x * x_local, count_y * y_local
    half = depth // 2
    slices = half // devices
    pack = LANES // x_local
    span = GROUP * pack
    groups = y_local // span
    cell_total = float(grid_x * grid_y * depth)
    lengths = sorted({grid_x, grid_y, depth})
    d1, d2, *refs = refs
    tables = {length: (refs[2 * n], refs[2 * n + 1]) for n, length in enumerate(lengths)}
    (back, partial, z1, z2, r1, r2, bs,
     dt, zt, rxh, rxl, ryh, ryl, xh, xl, lh, ll, spec, ph, plo, gh, gl, bt, pf, early_rows, early_table, turned, block,
     local, sent, got) = refs[2 * len(lengths) :]
    (yc_, ycl), (zc, zcl) = tables[grid_y], tables[depth]
    gx, gy = lax.axis_index("gx"), lax.axis_index("gy")
    me = gx * count_y + gy

    def peer(offset):
        dest = lax.rem(me + offset, devices)
        return dest, (dest // count_y, lax.rem(dest, count_y))

    barrier = pltpu.get_barrier_semaphore()

    def greet(offset, _):
        pl.semaphore_signal(barrier, inc=1, device_id=peer(offset)[1], device_id_type=MESH)
        return 0

    lax.fori_loop(1, devices, greet, 0)

    def local_copy(src, dst):
        copy = pltpu.make_async_copy(src, dst, local)
        copy.start()
        copy.wait()

    def send_all(source, target, sem):
        own = pltpu.make_async_copy(source(me), target, got.at[sem])
        own.start()

        def one(offset, _):
            dest, where = peer(offset)
            pltpu.make_async_remote_copy(
                source(dest), target, sent.at[sem], got.at[sem],
                device_id=where, device_id_type=MESH,
            ).start()
            return 0

        lax.fori_loop(1, devices, one, 0)

    def wait_bytes(ref, sem):
        pltpu.make_async_copy(ref, ref, sem).wait()

    rows_all = slices * devices * 2 * GROUP
    depth_tiles = depth // LANES

    def load_cells(density, group):
        for tile in range(depth_tiles):
            pltpu.make_async_copy(
                density.at[:, pl.ds(group * span, span), pl.ds(tile * LANES, LANES)], dt.at[tile], local
            ).start()
        pltpu.make_async_copy(dt, dt, local).wait()

    lines = dt.reshape(depth_tiles * x_local * span, LANES)
    packed_rows = zt.reshape(2 * rows_all, LANES)

    def forward_group(step, _):
        group = lax.rem(step, groups)

        @pl.when(step < groups)
        def _():
            load_cells(d1, group)

        @pl.when(step >= groups)
        def _():
            load_cells(d2, group)

        slot = jnp.minimum(step, 1)
        for first in range(0, GROUP, 2):
            cells = jnp.concatenate(
                [
                    jnp.concatenate(
                        [
                            lines[pl.ds(tile * x_local * span + h * GROUP + row, x_local, stride=span), :]
                            for tile in range(depth_tiles)
                        ],
                        axis=1,
                    )
                    for row in (first, first + 1)
                    for h in range(pack)
                ],
                axis=0,
            )
            cells = split(cells)
            for c in range(2):
                table = (zc[c * depth : c * depth + half, :], zcl[c * depth : c * depth + half, :])
                rows = dot3(table, cells, ((1,), (1,)))
                if c:
                    rows = -rows
                for n in range(2):
                    packed_rows[
                        pl.ds(slot * rows_all + c * GROUP + first + n, half, stride=2 * GROUP), :
                    ] = rows[:, n * LANES : (n + 1) * LANES]

        @pl.when(step == 0)
        def _():
            pl.semaphore_wait(barrier, devices - 1)
            send_all(lambda dest: zt.at[0, :, dest], r1.at[:, me, 0], 0)

        @pl.when((step > 0) & (step < groups))
        def _():
            local_copy(zt.at[1], z1.at[:, :, group])
            send_all(lambda dest: z1.at[:, dest, group], r1.at[:, me, group], group)

        @pl.when(step >= groups)
        def _():
            local_copy(zt.at[1], z2.at[:, :, group])

        return 0

    lax.fori_loop(0, 2 * groups, forward_group, 0)
    build_rotation(tables[grid_x], (rxh, rxl), grid_x, True)
    build_rotation(tables[grid_y], (ryh, ryl), grid_y, False)

    def unpack_rows(block):
        if pack > 1:
            block = jnp.concatenate(
                [
                    block[..., h * x_local : (h + 1) * x_local].reshape(count_y, groups, 1, GROUP, x_local)
                    for h in range(pack)
                ],
                axis=2,
            )
        return block.reshape(grid_y, x_local)

    def pack_rows(block):
        if pack == 1:
            return block.reshape(count_y, groups, GROUP, x_local)
        block = block.reshape(count_y, groups, pack, GROUP, x_local)
        return jnp.concatenate([block[:, :, h] for h in range(pack)], axis=-1)

    waited = 0
    for k in range(slices):
        upto = (k + 1) * groups // slices
        for group in range(waited, upto):
            wait_bytes(r1.at[:, :, group], got.at[group])
        waited = upto
        send_all(lambda dest: z2.at[k, dest], r2.at[k, me], groups + k)

    tile_x = min(256, grid_x)
    tile_y = min(256, grid_y)
    ky = lax.broadcasted_iota(jnp.int32, (grid_y, grid_x), 0)
    kx = lax.broadcasted_iota(jnp.int32, (grid_y, grid_x), 1)
    keep = (ky != grid_y // 2) & (kx != grid_x // 2)

    def plane(k, _):
        wait_bytes(r2.at[k], got.at[groups + k])
        local_copy(r1.at[k], pf.at[0])
        local_copy(r2.at[k], pf.at[1])
        def forward(field, _):
            cells = pf.at[field].reshape(count_x, count_y, groups, 2, GROUP, LANES)
            for c in range(2):
                for i in range(count_x):
                    high, low = split(unpack_rows(cells[i, :, :, c]))
                    at = c * grid_x + i * x_local
                    xh[:, at : at + x_local] = high
                    xl[:, at : at + x_local] = low
            for n in range(2 * grid_x // tile_x):
                cols = slice(n * tile_x, (n + 1) * tile_x)
                part = dot3((xh[...], xl[...]), (rxh[:, cols], rxl[:, cols]), ((1,), (0,)))
                c, at = divmod(n * tile_x, grid_x)
                high, low = split(part)
                lh[c * grid_y : (c + 1) * grid_y, at : at + tile_x] = high
                ll[c * grid_y : (c + 1) * grid_y, at : at + tile_x] = low
            for m in range(2 * grid_y // tile_y):
                rows = slice(m * tile_y, (m + 1) * tile_y)
                spec[field, rows, :] = dot3((ryh[rows, :], ryl[rows, :]), (lh[...], ll[...]), ((1,), (0,)))
            return 0

        lax.fori_loop(0, 2, forward, 0)
        power = spec[0, 0:grid_y] * spec[1, 0:grid_y] + spec[0, grid_y:] * spec[1, grid_y:]
        weight = jnp.where((k == 0) & (me == 0), 1.0, 2.0).astype(f32) * (1.0 / math.sqrt(cell_total))
        power = jnp.where(keep, power / cell_total, 0.0) * weight
        ph[...], plo[...] = split(power)
        for m in range(2 * grid_y // tile_y):
            rows = slice(m * tile_y, (m + 1) * tile_y)
            part = dot3((yc_[rows, :], ycl[rows, :]), (ph[...], plo[...]), ((1,), (0,)))
            c, at = divmod(m * tile_y, grid_y)
            high, low = split(part)
            gh[at : at + tile_y, c * grid_x : (c + 1) * grid_x] = high
            gl[at : at + tile_y, c * grid_x : (c + 1) * grid_x] = low
        cells = bt.reshape(count_x, count_y, groups, 2, GROUP, LANES)
        for n in range(2 * grid_x // tile_x):
            rows = slice(n * tile_x, (n + 1) * tile_x)
            part = dot3((gh[...], gl[...]), (rxh[rows, :], rxl[rows, :]), ((1,), (1,)))
            c, at = divmod(n * tile_x, grid_x)
            for m in range(tile_x // x_local):
                i = at // x_local + m
                cells[i, :, :, c] = pack_rows(part[:, m * x_local : (m + 1) * x_local])
        local_copy(bt, bs.at[k])
        send_all(lambda dest: bs.at[k, dest], back.at[k, me], groups + slices + k)
        return 0

    lax.fori_loop(0, slices, plane, 0)
    tail = tail_slices(slices)
    early = slices - tail
    for k in range(early):
        wait_bytes(back.at[k], got.at[groups + slices + k])
    if early:
        count = early * devices
        for part in range(2):
            table = tables[depth][part]
            early_table[part, 0:count, :] = table[0:count, :]
            early_table[part, count : 2 * count, :] = -table[depth : depth + count, :]
        early_lines = early_rows.reshape(count * 2 * GROUP, LANES)
        early_out = turned.reshape(2 * count // LANES * x_local * span, LANES)
        block_rows = block.reshape(x_local * span, depth)
        height = min(256, x_local * span)

        def early_group(group, _):
            local_copy(back.at[pl.ds(0, early), :, group], early_rows)
            interleave(early_lines, count, x_local, span, early_out)

            def strip(m, _):
                rows = pl.ds(pl.multiple_of(m * height, height), height)
                block_rows[rows, :] = dot3(
                    interleaved_rows(turned, rows), (early_table[0], early_table[1]), ((1,), (0,))
                )
                return 0

            lax.fori_loop(0, x_local * span // height, strip, 0)
            local_copy(block, partial.at[:, pl.ds(pl.multiple_of(group * span, span), span), :])
            return 0

        lax.fori_loop(0, groups, early_group, 0)
    for k in range(early, slices):
        wait_bytes(back.at[k], got.at[groups + slices + k])
    wait_bytes(zt.at[0, :, pl.ds(0, devices - 1)], sent.at[0])
    for group in range(1, groups):
        wait_bytes(z1.at[:, pl.ds(0, devices - 1), group], sent.at[group])
    for k in range(slices):
        wait_bytes(z2.at[k, pl.ds(0, devices - 1)], sent.at[groups + k])
        wait_bytes(bs.at[k, pl.ds(0, devices - 1)], sent.at[groups + slices + k])


def depth_inverse_kernel(has_partial, rows_ref, ch, cl, sh, sl, partial_ref, out_ref, turned, table):
    x_local, span, depth = out_ref.shape
    tail, devices = rows_ref.shape[:2]
    count = tail * devices
    lines = rows_ref.reshape(count * 2 * GROUP, LANES)

    @pl.when(pl.program_id(0) == 0)
    def _():
        for n, part in enumerate((ch[...], -sh[...], cl[...], -sl[...], ch[...], -sh[...])):
            table[n * count : (n + 1) * count, :] = part

    interleave(lines, count, x_local, span, turned.reshape(turned.shape[0] * x_local * span, LANES))
    out = out_ref.reshape(x_local * span, depth)
    partial = partial_ref.reshape(x_local * span, depth)
    height = min(512, x_local * span)
    for m in range(x_local * span // height):
        rows = slice(m * height, (m + 1) * height)
        high, low = interleaved_rows(turned, rows)
        total = lax.dot_general(
            jnp.concatenate([high, high, low], axis=1), table[...], (((1,), (0,)), ((), ())), preferred_element_type=f32
        )
        out[rows, :] = total + partial[rows, :] if has_partial else total


def on_device(density_one, density_two):
    count_x = lax.axis_size("gx")
    count_y = lax.axis_size("gy")
    devices = count_x * count_y
    x_local, y_local, depth = density_one.shape
    grid_x, grid_y = x_local * count_x, y_local * count_y
    slices = depth // 2 // devices
    span = GROUP * (LANES // x_local)
    groups = y_local // span
    tail = tail_slices(slices)
    early = slices - tail
    lengths = sorted({grid_x, grid_y, depth})
    tables = {length: halves(trig(length)) for length in lengths}
    packed = jax.ShapeDtypeStruct((slices, devices, groups, 2 * GROUP, LANES), f32)
    vmem = pl.BlockSpec(memory_space=pltpu.VMEM)
    hbm = pl.BlockSpec(memory_space=pl.ANY)
    scratch = [
        pltpu.VMEM((depth // LANES, x_local, span, LANES), f32),
        pltpu.VMEM((2, slices, devices, 2 * GROUP, LANES), f32),
        pltpu.VMEM((2 * grid_x, 2 * grid_x), bf16),
        pltpu.VMEM((2 * grid_x, 2 * grid_x), bf16),
        pltpu.VMEM((2 * grid_y, 2 * grid_y), bf16),
        pltpu.VMEM((2 * grid_y, 2 * grid_y), bf16),
        pltpu.VMEM((grid_y, 2 * grid_x), bf16),
        pltpu.VMEM((grid_y, 2 * grid_x), bf16),
        pltpu.VMEM((2 * grid_y, grid_x), bf16),
        pltpu.VMEM((2 * grid_y, grid_x), bf16),
        pltpu.VMEM((2, 2 * grid_y, grid_x), f32),
        pltpu.VMEM((grid_y, grid_x), bf16),
        pltpu.VMEM((grid_y, grid_x), bf16),
        pltpu.VMEM((grid_y, 2 * grid_x), bf16),
        pltpu.VMEM((grid_y, 2 * grid_x), bf16),
        pltpu.VMEM((devices, groups, 2 * GROUP, LANES), f32),
        pltpu.VMEM((2, devices, groups, 2 * GROUP, LANES), f32),
        pltpu.VMEM((max(1, early), devices, 2 * GROUP, LANES), f32),
        pltpu.VMEM((2, max(1, early) * devices * 2, depth), bf16),
        pltpu.VMEM((max(1, early) * devices * 2 // LANES, x_local * span, LANES), f32),
        pltpu.VMEM((x_local, span, depth), f32),
        pltpu.SemaphoreType.DMA,
        pltpu.SemaphoreType.DMA((groups + 2 * slices,)),
        pltpu.SemaphoreType.DMA((groups + 2 * slices,)),
    ]
    sizes = (count_x, count_y, x_local, y_local, depth)
    back, partial = pl.pallas_call(
        functools.partial(exchange_kernel, sizes),
        out_shape=[packed, jax.ShapeDtypeStruct(density_one.shape, f32)] + [packed] * 5,
        in_specs=[hbm] * 2 + [vmem] * (2 * len(lengths)),
        out_specs=[hbm] * 7,
        scratch_shapes=scratch,
        compiler_params=pltpu.CompilerParams(
            collective_id=0, has_side_effects=True, vmem_limit_bytes=60 * 2**20
        ),
    )(density_one, density_two, *(part for length in lengths for part in tables[length]))[:2]
    count = tail * devices
    cosines = pl.BlockSpec((count, depth), lambda g: (early // tail, 0))
    sines = pl.BlockSpec((count, depth), lambda g: (depth // count + early // tail, 0))
    high, low = tables[depth]
    block = pl.BlockSpec((x_local, span, depth), lambda g: (0, g, 0))
    return pl.pallas_call(
        functools.partial(depth_inverse_kernel, early > 0),
        grid=(groups,),
        out_shape=jax.ShapeDtypeStruct(density_one.shape, f32),
        in_specs=[
            pl.BlockSpec((tail, devices, 1, 2 * GROUP, LANES), lambda g: (early // tail, 0, g, 0, 0)),
            cosines,
            cosines,
            sines,
            sines,
            block,
        ],
        out_specs=block,
        scratch_shapes=[
            pltpu.VMEM((2 * count // LANES, x_local * span, LANES), f32),
            pltpu.VMEM((6 * count, depth), bf16),
        ],
        compiler_params=pltpu.CompilerParams(vmem_limit_bytes=48 * 2**20),
    )(back, high, low, high, low, partial)


def solution(mesh):
    return jax.shard_map(
        on_device,
        mesh=mesh,
        in_specs=(P("gx", "gy", None), P("gx", "gy", None)),
        out_specs=P("gx", "gy", None),
        check_vma=False,
    )
```

```python
import functools
import math

import jax
import jax.numpy as jnp
import numpy as np
from jax import lax
from jax.experimental import pallas as pl
from jax.experimental.pallas import tpu as pltpu
from jax.sharding import PartitionSpec as P

MESH = pl.DeviceIdType.MESH
GROUP = 8
LANES = 128
f32 = jnp.float32
bf16 = jnp.bfloat16


def trig(length):
    positions = np.arange(length)
    radians = (positions[:, None] * positions[None, :] % length) * (2.0 * math.pi / length)
    return np.concatenate([np.cos(radians), np.sin(radians)]).astype(np.float32)


def halves(table):
    table = jnp.asarray(table)
    high = table.astype(bf16)
    low = (table - high.astype(f32)).astype(bf16)
    return high, low


def split(values):
    high = values.astype(bf16)
    return high, (values - high.astype(f32)).astype(bf16)


def dot3(left, right, contract):
    def one(a, b):
        return lax.dot_general(a, b, (contract, ((), ())), preferred_element_type=f32)

    (lh, ll), (rh, rl) = left, right
    return one(lh, rh) + one(lh, rl) + one(ll, rh)


def build_rotation(table, out, size, right):
    for part in range(2):
        cos = table[part][0:size, :]
        sin = table[part][size : 2 * size, :]
        out[part][0:size, 0:size] = cos
        out[part][size : 2 * size, size : 2 * size] = cos
        out[part][0:size, size : 2 * size] = -sin if right else sin
        out[part][size : 2 * size, 0:size] = sin if right else -sin


def interleave(lines, count, x_local, span, out, base=0):
    for row in range(GROUP):
        cells = jnp.concatenate(
            [lines[pl.ds(base + c * GROUP + row, count, stride=2 * GROUP), :] for c in range(2)], axis=0
        ).T
        for h in range(span // GROUP):
            for tile in range(2 * count // LANES):
                out[pl.ds(tile * x_local * span + h * GROUP + row, x_local, stride=span), :] = cells[
                    h * x_local : (h + 1) * x_local, tile * LANES : (tile + 1) * LANES
                ]


def interleaved_rows(lines, rows):
    return split(jnp.concatenate([lines[tile, rows, :] for tile in range(lines.shape[0])], axis=1))


def tail_slices(slices):
    return max(1, slices // 4)


def exchange_kernel(sizes, *refs):
    count_x, count_y, x_local, y_local, depth = sizes
    devices = count_x * count_y
    grid_x, grid_y = count_x * x_local, count_y * y_local
    half = depth // 2
    slices = half // devices
    pack = LANES // x_local
    span = GROUP * pack
    groups = y_local // span
    cell_total = float(grid_x * grid_y * depth)
    lengths = sorted({grid_x, grid_y, depth})
    d1, d2, *refs = refs
    tables = {length: (refs[2 * n], refs[2 * n + 1]) for n, length in enumerate(lengths)}
    (back, partial, z1, z2, r1, r2, bs,
     dt, zt, rxh, rxl, ryh, ryl, xh, xl, lh, ll, spec, ph, plo, gh, gl, bt, pf, early_rows, early_table, turned, block,
     local, sent, got, fetched, written) = refs[2 * len(lengths) :]
    (yc_, ycl), (zc, zcl) = tables[grid_y], tables[depth]
    gx, gy = lax.axis_index("gx"), lax.axis_index("gy")
    me = gx * count_y + gy

    def peer(offset):
        dest = lax.rem(me + offset, devices)
        return dest, (dest // count_y, lax.rem(dest, count_y))

    barrier = pltpu.get_barrier_semaphore()

    def greet(offset, _):
        pl.semaphore_signal(barrier, inc=1, device_id=peer(offset)[1], device_id_type=MESH)
        return 0

    lax.fori_loop(1, devices, greet, 0)

    def local_copy(src, dst):
        copy = pltpu.make_async_copy(src, dst, local)
        copy.start()
        copy.wait()

    def send_all(source, target, sem):
        own = pltpu.make_async_copy(source(me), target, got.at[sem])
        own.start()

        def one(offset, _):
            dest, where = peer(offset)
            pltpu.make_async_remote_copy(
                source(dest), target, sent.at[sem], got.at[sem],
                device_id=where, device_id_type=MESH,
            ).start()
            return 0

        lax.fori_loop(1, devices, one, 0)

    def wait_bytes(ref, sem):
        pltpu.make_async_copy(ref, ref, sem).wait()

    rows_all = slices * devices * 2 * GROUP
    depth_tiles = depth // LANES

    def load_cells(density, group):
        for tile in range(depth_tiles):
            pltpu.make_async_copy(
                density.at[:, pl.ds(group * span, span), pl.ds(tile * LANES, LANES)], dt.at[tile], local
            ).start()
        pltpu.make_async_copy(dt, dt, local).wait()

    lines = dt.reshape(depth_tiles * x_local * span, LANES)
    packed_rows = zt.reshape(2 * rows_all, LANES)

    def forward_group(step, _):
        group = lax.rem(step, groups)

        @pl.when(step < groups)
        def _():
            load_cells(d1, group)

        @pl.when(step >= groups)
        def _():
            load_cells(d2, group)

        slot = jnp.minimum(step, 1)
        for first in range(0, GROUP, 2):
            cells = jnp.concatenate(
                [
                    jnp.concatenate(
                        [
                            lines[pl.ds(tile * x_local * span + h * GROUP + row, x_local, stride=span), :]
                            for tile in range(depth_tiles)
                        ],
                        axis=1,
                    )
                    for row in (first, first + 1)
                    for h in range(pack)
                ],
                axis=0,
            )
            cells = split(cells)
            for c in range(2):
                table = (zc[c * depth : c * depth + half, :], zcl[c * depth : c * depth + half, :])
                rows = dot3(table, cells, ((1,), (1,)))
                if c:
                    rows = -rows
                for n in range(2):
                    packed_rows[
                        pl.ds(slot * rows_all + c * GROUP + first + n, half, stride=2 * GROUP), :
                    ] = rows[:, n * LANES : (n + 1) * LANES]

        @pl.when(step == 0)
        def _():
            pl.semaphore_wait(barrier, devices - 1)
            send_all(lambda dest: zt.at[0, :, dest], r1.at[:, me, 0], 0)

        @pl.when((step > 0) & (step < groups))
        def _():
            local_copy(zt.at[1], z1.at[:, :, group])
            send_all(lambda dest: z1.at[:, dest, group], r1.at[:, me, group], group)

        @pl.when(step >= groups)
        def _():
            local_copy(zt.at[1], z2.at[:, :, group])

        return 0

    lax.fori_loop(0, 2 * groups, forward_group, 0)
    build_rotation(tables[grid_x], (rxh, rxl), grid_x, True)
    build_rotation(tables[grid_y], (ryh, ryl), grid_y, False)

    def unpack_rows(block):
        if pack > 1:
            block = jnp.concatenate(
                [
                    block[..., h * x_local : (h + 1) * x_local].reshape(count_y, groups, 1, GROUP, x_local)
                    for h in range(pack)
                ],
                axis=2,
            )
        return block.reshape(grid_y, x_local)

    def pack_rows(block):
        if pack == 1:
            return block.reshape(count_y, groups, GROUP, x_local)
        block = block.reshape(count_y, groups, pack, GROUP, x_local)
        return jnp.concatenate([block[:, :, h] for h in range(pack)], axis=-1)

    waited = 0
    for k in range(slices):
        upto = (k + 1) * groups // slices
        for group in range(waited, upto):
            wait_bytes(r1.at[:, :, group], got.at[group])
        waited = upto
        send_all(lambda dest: z2.at[k, dest], r2.at[k, me], groups + k)

    tile_x = min(256, grid_x)
    tile_y = min(256, grid_y)
    ky = lax.broadcasted_iota(jnp.int32, (grid_y, grid_x), 0)
    kx = lax.broadcasted_iota(jnp.int32, (grid_y, grid_x), 1)
    keep = (ky != grid_y // 2) & (kx != grid_x // 2)

    def plane(k, _):
        wait_bytes(r2.at[k], got.at[groups + k])
        local_copy(r1.at[k], pf.at[0])
        local_copy(r2.at[k], pf.at[1])
        def forward(field, _):
            cells = pf.at[field].reshape(count_x, count_y, groups, 2, GROUP, LANES)
            for c in range(2):
                for i in range(count_x):
                    high, low = split(unpack_rows(cells[i, :, :, c]))
                    at = c * grid_x + i * x_local
                    xh[:, at : at + x_local] = high
                    xl[:, at : at + x_local] = low
            for n in range(2 * grid_x // tile_x):
                cols = slice(n * tile_x, (n + 1) * tile_x)
                part = dot3((xh[...], xl[...]), (rxh[:, cols], rxl[:, cols]), ((1,), (0,)))
                c, at = divmod(n * tile_x, grid_x)
                high, low = split(part)
                lh[c * grid_y : (c + 1) * grid_y, at : at + tile_x] = high
                ll[c * grid_y : (c + 1) * grid_y, at : at + tile_x] = low
            for m in range(2 * grid_y // tile_y):
                rows = slice(m * tile_y, (m + 1) * tile_y)
                spec[field, rows, :] = dot3((ryh[rows, :], ryl[rows, :]), (lh[...], ll[...]), ((1,), (0,)))
            return 0

        lax.fori_loop(0, 2, forward, 0)
        power = spec[0, 0:grid_y] * spec[1, 0:grid_y] + spec[0, grid_y:] * spec[1, grid_y:]
        weight = jnp.where((k == 0) & (me == 0), 1.0, 2.0).astype(f32) * (1.0 / math.sqrt(cell_total))
        power = jnp.where(keep, power / cell_total, 0.0) * weight
        ph[...], plo[...] = split(power)
        for m in range(2 * grid_y // tile_y):
            rows = slice(m * tile_y, (m + 1) * tile_y)
            part = dot3((yc_[rows, :], ycl[rows, :]), (ph[...], plo[...]), ((1,), (0,)))
            c, at = divmod(m * tile_y, grid_y)
            high, low = split(part)
            gh[at : at + tile_y, c * grid_x : (c + 1) * grid_x] = high
            gl[at : at + tile_y, c * grid_x : (c + 1) * grid_x] = low
        cells = bt.reshape(count_x, count_y, groups, 2, GROUP, LANES)
        for n in range(2 * grid_x // tile_x):
            rows = slice(n * tile_x, (n + 1) * tile_x)
            part = dot3((gh[...], gl[...]), (rxh[rows, :], rxl[rows, :]), ((1,), (1,)))
            c, at = divmod(n * tile_x, grid_x)
            for m in range(tile_x // x_local):
                i = at // x_local + m
                cells[i, :, :, c] = pack_rows(part[:, m * x_local : (m + 1) * x_local])
        local_copy(bt, bs.at[k])
        send_all(lambda dest: bs.at[k, dest], back.at[k, me], groups + slices + k)
        return 0

    lax.fori_loop(0, slices, plane, 0)
    tail = tail_slices(slices)
    early = slices - tail
    for k in range(early):
        wait_bytes(back.at[k], got.at[groups + slices + k])
    if early:
        count = early * devices
        for part in range(2):
            table = tables[depth][part]
            early_table[part, 0:count, :] = table[0:count, :]
            early_table[part, count : 2 * count, :] = -table[depth : depth + count, :]
        row_count = count * 2 * GROUP
        cell_count = x_local * span
        early_lines = early_rows.reshape(2 * row_count, LANES)
        early_out = turned.reshape(2 * count // LANES * cell_count, LANES)
        block_rows = block.reshape(2 * cell_count, depth)
        height = min(256, cell_count)

        def fetch(group, slot):
            return pltpu.make_async_copy(
                back.at[pl.ds(0, early), :, group], early_rows.at[slot], fetched.at[slot]
            )

        def stored(slot):
            pltpu.make_async_copy(block.at[slot], block.at[slot], written.at[slot]).wait()

        fetch(0, 0).start()

        def early_group(group, _):
            slot = lax.rem(group, 2)
            fetch(group, slot).wait()

            @pl.when(group < groups - 1)
            def _():
                fetch(group + 1, 1 - slot).start()

            @pl.when(group >= 2)
            def _():
                stored(slot)

            interleave(early_lines, count, x_local, span, early_out, slot * row_count)

            def strip(m, _):
                rows = pl.ds(pl.multiple_of(m * height, height), height)
                target = pl.ds(pl.multiple_of(slot * cell_count + m * height, height), height)
                block_rows[target, :] = dot3(
                    interleaved_rows(turned, rows), (early_table[0], early_table[1]), ((1,), (0,))
                )
                return 0

            lax.fori_loop(0, cell_count // height, strip, 0)
            pltpu.make_async_copy(
                block.at[slot],
                partial.at[:, pl.ds(pl.multiple_of(group * span, span), span), :],
                written.at[slot],
            ).start()
            return 0

        lax.fori_loop(0, groups, early_group, 0)
        for slot in range(min(2, groups)):
            stored(slot)
    for k in range(early, slices):
        wait_bytes(back.at[k], got.at[groups + slices + k])
    wait_bytes(zt.at[0, :, pl.ds(0, devices - 1)], sent.at[0])
    for group in range(1, groups):
        wait_bytes(z1.at[:, pl.ds(0, devices - 1), group], sent.at[group])
    for k in range(slices):
        wait_bytes(z2.at[k, pl.ds(0, devices - 1)], sent.at[groups + k])
        wait_bytes(bs.at[k, pl.ds(0, devices - 1)], sent.at[groups + slices + k])


def depth_inverse_kernel(
    early, back, high, low, partial, out, lines, cells, turned, parts, table, tables_in, lines_in, cells_in, cells_out
):
    groups, x_local, span, depth = cells.shape
    tail, devices = lines.shape[1:3]
    count = tail * devices
    sources = [
        part.at[pl.ds(c * depth + early * devices, count), :] for part in (high, low) for c in range(2)
    ]
    for n, source in enumerate(sources):
        pltpu.make_async_copy(source, parts.at[n], tables_in).start()

    def fetch(group):
        copies = [
            pltpu.make_async_copy(back.at[pl.ds(early, tail), :, group], lines.at[group], lines_in.at[group])
        ]
        if early:
            at = pl.ds(group * span, span)
            copies.append(pltpu.make_async_copy(partial.at[:, at, :], cells.at[group], cells_in.at[group]))
        return copies

    for group in range(groups):
        for copy in fetch(group):
            copy.start()
    pltpu.make_async_copy(parts, parts, tables_in).wait()
    for n, part in enumerate((parts[0], -parts[1], parts[2], -parts[3], parts[0], -parts[1])):
        table[n * count : (n + 1) * count, :] = part
    row_count = count * 2 * GROUP
    cell_count = x_local * span
    all_lines = lines.reshape(groups * row_count, LANES)
    all_cells = cells.reshape(groups * cell_count, depth)
    height = min(512, cell_count)

    def one(group, _):
        pltpu.make_async_copy(lines.at[group], lines.at[group], lines_in.at[group]).wait()
        interleave(
            all_lines, count, x_local, span, turned.reshape(turned.shape[0] * cell_count, LANES), group * row_count
        )
        if early:
            pltpu.make_async_copy(cells.at[group], cells.at[group], cells_in.at[group]).wait()
        for m in range(cell_count // height):
            high, low = interleaved_rows(turned, slice(m * height, (m + 1) * height))
            total = lax.dot_general(
                jnp.concatenate([high, high, low], axis=1),
                table[...],
                (((1,), (0,)), ((), ())),
                preferred_element_type=f32,
            )
            rows = pl.ds(pl.multiple_of(group * cell_count + m * height, height), height)
            all_cells[rows, :] = total + all_cells[rows, :] if early else total
        pltpu.make_async_copy(
            cells.at[group], out.at[:, pl.ds(pl.multiple_of(group * span, span), span), :], cells_out
        ).start()
        return 0

    lax.fori_loop(0, groups, one, 0)
    pltpu.make_async_copy(cells, cells, cells_out).wait()


def on_device(density_one, density_two):
    count_x = lax.axis_size("gx")
    count_y = lax.axis_size("gy")
    devices = count_x * count_y
    x_local, y_local, depth = density_one.shape
    grid_x, grid_y = x_local * count_x, y_local * count_y
    slices = depth // 2 // devices
    span = GROUP * (LANES // x_local)
    groups = y_local // span
    tail = tail_slices(slices)
    early = slices - tail
    lengths = sorted({grid_x, grid_y, depth})
    tables = {length: halves(trig(length)) for length in lengths}
    packed = jax.ShapeDtypeStruct((slices, devices, groups, 2 * GROUP, LANES), f32)
    vmem = pl.BlockSpec(memory_space=pltpu.VMEM)
    hbm = pl.BlockSpec(memory_space=pl.ANY)
    scratch = [
        pltpu.VMEM((depth // LANES, x_local, span, LANES), f32),
        pltpu.VMEM((2, slices, devices, 2 * GROUP, LANES), f32),
        pltpu.VMEM((2 * grid_x, 2 * grid_x), bf16),
        pltpu.VMEM((2 * grid_x, 2 * grid_x), bf16),
        pltpu.VMEM((2 * grid_y, 2 * grid_y), bf16),
        pltpu.VMEM((2 * grid_y, 2 * grid_y), bf16),
        pltpu.VMEM((grid_y, 2 * grid_x), bf16),
        pltpu.VMEM((grid_y, 2 * grid_x), bf16),
        pltpu.VMEM((2 * grid_y, grid_x), bf16),
        pltpu.VMEM((2 * grid_y, grid_x), bf16),
        pltpu.VMEM((2, 2 * grid_y, grid_x), f32),
        pltpu.VMEM((grid_y, grid_x), bf16),
        pltpu.VMEM((grid_y, grid_x), bf16),
        pltpu.VMEM((grid_y, 2 * grid_x), bf16),
        pltpu.VMEM((grid_y, 2 * grid_x), bf16),
        pltpu.VMEM((devices, groups, 2 * GROUP, LANES), f32),
        pltpu.VMEM((2, devices, groups, 2 * GROUP, LANES), f32),
        pltpu.VMEM((2, max(1, early), devices, 2 * GROUP, LANES), f32),
        pltpu.VMEM((2, max(1, early) * devices * 2, depth), bf16),
        pltpu.VMEM((max(1, early) * devices * 2 // LANES, x_local * span, LANES), f32),
        pltpu.VMEM((2, x_local, span, depth), f32),
        pltpu.SemaphoreType.DMA,
        pltpu.SemaphoreType.DMA((groups + 2 * slices,)),
        pltpu.SemaphoreType.DMA((groups + 2 * slices,)),
        pltpu.SemaphoreType.DMA((2,)),
        pltpu.SemaphoreType.DMA((2,)),
    ]
    sizes = (count_x, count_y, x_local, y_local, depth)
    back, partial = pl.pallas_call(
        functools.partial(exchange_kernel, sizes),
        out_shape=[packed, jax.ShapeDtypeStruct(density_one.shape, f32)] + [packed] * 5,
        in_specs=[hbm] * 2 + [vmem] * (2 * len(lengths)),
        out_specs=[hbm] * 7,
        scratch_shapes=scratch,
        compiler_params=pltpu.CompilerParams(
            collective_id=0, has_side_effects=True, vmem_limit_bytes=60 * 2**20
        ),
    )(density_one, density_two, *(part for length in lengths for part in tables[length]))[:2]
    count = tail * devices
    return pl.pallas_call(
        functools.partial(depth_inverse_kernel, early),
        out_shape=jax.ShapeDtypeStruct(density_one.shape, f32),
        in_specs=[hbm] * 4,
        out_specs=hbm,
        scratch_shapes=[
            pltpu.VMEM((groups, tail, devices, 2 * GROUP, LANES), f32),
            pltpu.VMEM((groups, x_local, span, depth), f32),
            pltpu.VMEM((2 * count // LANES, x_local * span, LANES), f32),
            pltpu.VMEM((4, count, depth), bf16),
            pltpu.VMEM((6 * count, depth), bf16),
            pltpu.SemaphoreType.DMA,
            pltpu.SemaphoreType.DMA((groups,)),
            pltpu.SemaphoreType.DMA((groups,)),
            pltpu.SemaphoreType.DMA,
        ],
        compiler_params=pltpu.CompilerParams(vmem_limit_bytes=60 * 2**20),
    )(back, *tables[depth], partial)


def solution(mesh):
    return jax.shard_map(
        on_device,
        mesh=mesh,
        in_specs=(P("gx", "gy", None), P("gx", "gy", None)),
        out_specs=P("gx", "gy", None),
        check_vma=False,
    )
```
